32 devices in a mesh: batch: 4 (over y, x), feat: 8 (over z, core).
Axes of the slice: x: 2, y: 2, z: 4, core: 2. Of those that a mesh axis runs over, the one named last changes fastest.
Arguments:
- view_a: bfloat16 [1024, 8192], P('batch', 'feat'), may hold values from -16 to 16
- view_b: bfloat16 [1024, 8192], P('batch', 'feat'), may hold values from -16 to 16
Outputs:
- loss_value: float32 [], replicated
- grad_a: float32 [1024, 8192], P('batch', 'feat')
- grad_b: float32 [1024, 8192], P('batch', 'feat')
The draws below stay inside these ranges and needn't reach their ends.
All inputs are finite; a program needn't handle non-finite values.
Results may differ from the reference program's by a relative error of at most 0.0026.
Values may be sent and summed in bfloat16 or wider, within the bound.
A program may use at most 64 MiB of HBM per device.

```python
import math
import jax
import jax.numpy as jnp
from jax import lax

F = 8192
BATCH = 1024


def common_signal(key):
    base = jax.random.normal(jax.random.fold_in(key, 102), (BATCH, F), jnp.float32)
    factors = jax.random.normal(jax.random.fold_in(key, 103), (BATCH, 32), jnp.float32)
    loadings = 0.25 * jax.random.normal(jax.random.fold_in(key, 104), (32, F), jnp.float32)
    return base + jnp.dot(factors, loadings, precision=lax.Precision.HIGHEST)


def shaped_view(key, salt):
    common = common_signal(key)
    noise = jax.random.normal(jax.random.fold_in(key, salt), (BATCH, F), jnp.float32)
    spread = math.log(2.0)
    factor = jnp.exp(jax.random.uniform(jax.random.fold_in(key, salt + 1), (F,), jnp.float32, -spread, spread))
    offset = jax.random.uniform(jax.random.fold_in(key, salt + 2), (F,), jnp.float32, -2.0, 2.0)
    drift = jax.random.uniform(jax.random.fold_in(key, salt + 3), (F,), jnp.float32, -1.0, 1.0)
    ramp = 2.0 * (jnp.arange(BATCH, dtype=jnp.float32) + 0.5) / BATCH - 1.0
    values = (common + 0.8 * noise) * factor + offset + drift * ramp[:, None]
    return jnp.clip(values, -16.0, 16.0).astype(jnp.bfloat16)


def draw_view_a(key, part):
    return shaped_view(key, 201)


def draw_view_b(key, part):
    return shaped_view(key, 301)


def setup_inputs(seed: int = 0) -> dict:
    streams_of = jax.random.split(jax.random.key(seed), 3)
    return {
        "view_a": draw_view_a(jax.random.fold_in(streams_of[2], 71), 0),
        "view_b": draw_view_b(jax.random.fold_in(streams_of[2], 71), 0),
    }


variance_floor = 0.25
redundancy = 0.0051

def normalize(view):
    values = view.astype(jnp.float32)
    center = lax.optimization_barrier(jnp.mean(values, axis=0))
    shifted = values - center
    variance = lax.optimization_barrier(jnp.mean(shifted * shifted, axis=0))
    factor = lax.rsqrt(variance + variance_floor)
    return (shifted * factor, factor)

def backward(dnorm, normed, factor):
    first = lax.optimization_barrier(jnp.mean(dnorm, axis=0))
    second = lax.optimization_barrier(jnp.mean(dnorm * normed, axis=0))
    return (dnorm - first - normed * second) * factor

def reference(view_a, view_b):
    normed_a, factor_a = normalize(view_a)
    normed_b, factor_b = normalize(view_b)
    low_a = normed_a.astype(jnp.bfloat16)
    low_b = normed_b.astype(jnp.bfloat16)
    batch_total, feature_total = view_a.shape
    block_cols = math.gcd(feature_total, 1024)
    blocks = feature_total // block_cols
    stacked_b = low_b.reshape(batch_total, blocks, block_cols).transpose(1, 0, 2)
    row_ids = jnp.arange(feature_total, dtype=jnp.int32)

    def advance(carry, inputs):
        grad_acc, loss_acc = carry
        part_b, number = inputs
        cross_block = lax.dot_general(low_a, part_b, (((0,), (0,)), ((), ())), preferred_element_type=jnp.float32) / batch_total
        col_ids = number * block_cols + jnp.arange(block_cols, dtype=jnp.int32)
        diagonal_mask = row_ids[:, None] == col_ids[None, :]
        missing = 1.0 - cross_block
        loss_acc = loss_acc + jnp.sum(jnp.where(diagonal_mask, missing * missing, redundancy * cross_block * cross_block))
        dcross = jnp.where(diagonal_mask, 2.0 * (cross_block - 1.0), 2.0 * redundancy * cross_block).astype(jnp.bfloat16)
        dnorm_part = jnp.dot(low_a, dcross, preferred_element_type=jnp.float32)
        grad_acc = grad_acc + lax.dot_general(part_b, dcross, (((1,), (1,)), ((), ())), preferred_element_type=jnp.float32)
        return ((grad_acc, loss_acc), dnorm_part)
    start = (jnp.zeros((batch_total, feature_total), jnp.float32), jnp.zeros((), jnp.float32))
    (dnorm_a, loss_sum), pieces = lax.scan(advance, start, (stacked_b, jnp.arange(blocks, dtype=jnp.int32)))
    dnorm_b = pieces.transpose(1, 0, 2).reshape(batch_total, feature_total)
    grad_a = backward(dnorm_a, normed_a, factor_a)
    grad_b = backward(dnorm_b, normed_b, factor_b)
    return (loss_sum / feature_total, grad_a, grad_b)
```

```python
import jax
import jax.numpy as jnp
from jax import lax
from jax.sharding import PartitionSpec as P

variance_floor = 0.25
redundancy = 0.0051


def local(view_a, view_b):
    rows_dev, cols_dev = view_a.shape
    groups = lax.axis_size("batch")
    batch_total = rows_dev * groups
    feature_total = cols_dev * lax.axis_size("feat")
    scale = 2.0 * redundancy / batch_total
    all_a = lax.all_gather(view_a, "batch", axis=0, tiled=True).astype(jnp.float32)
    all_b = lax.all_gather(view_b, "batch", axis=0, tiled=True).astype(jnp.float32)

    def normalize(values):
        shifted = values - jnp.mean(values, axis=0)
        factor = lax.rsqrt(jnp.mean(shifted * shifted, axis=0) + variance_floor)
        return shifted * factor, factor

    full_a, factor_a = normalize(all_a)
    full_b, factor_b = normalize(all_b)
    samples_a = full_a.astype(jnp.bfloat16)
    samples_b = full_b.astype(jnp.bfloat16)
    start = lax.axis_index("batch") * rows_dev
    normed_a = lax.dynamic_slice_in_dim(full_a, start, rows_dev)
    normed_b = lax.dynamic_slice_in_dim(full_b, start, rows_dev)
    low_a = normed_a.astype(jnp.bfloat16)
    low_b = normed_b.astype(jnp.bfloat16)
    diagonal = (
        jnp.sum(samples_a.astype(jnp.float32) * samples_b.astype(jnp.float32), axis=0)
        / batch_total
    )
    rows_t = (((1,), (1,)), ((), ()))
    gram_a = lax.dot_general(low_a, samples_a, rows_t, preferred_element_type=jnp.float32)
    gram_b = lax.dot_general(low_b, samples_b, rows_t, preferred_element_type=jnp.float32)
    gram_a, gram_b = lax.psum((gram_a, gram_b), "feat")
    square_sum = jnp.sum(gram_a * gram_b) / (batch_total * batch_total)
    missing = 1.0 - diagonal
    on_diagonal = jnp.sum(missing * missing - redundancy * diagonal * diagonal)
    loss_value = (
        redundancy * lax.psum(square_sum, "batch") + lax.psum(on_diagonal, "feat")
    ) / feature_total
    ddiag = (2.0 * (diagonal - 1.0)).astype(jnp.bfloat16).astype(jnp.float32)
    rest = ddiag - 2.0 * redundancy * diagonal
    dnorm_a = scale * jnp.dot(
        gram_b.astype(jnp.bfloat16), samples_a, preferred_element_type=jnp.float32
    ) + low_b.astype(jnp.float32) * rest
    dnorm_b = scale * jnp.dot(
        gram_a.astype(jnp.bfloat16), samples_b, preferred_element_type=jnp.float32
    ) + low_a.astype(jnp.float32) * rest
    grad_totals = lax.psum(
        jnp.stack([
            jnp.sum(dnorm_a, axis=0),
            jnp.sum(dnorm_a * normed_a, axis=0),
            jnp.sum(dnorm_b, axis=0),
            jnp.sum(dnorm_b * normed_b, axis=0),
        ]),
        "batch",
    ) / batch_total
    grad_a = (dnorm_a - grad_totals[0] - normed_a * grad_totals[1]) * factor_a
    grad_b = (dnorm_b - grad_totals[2] - normed_b * grad_totals[3]) * factor_b
    return (loss_value, grad_a, grad_b)


def solution(mesh):
    return jax.shard_map(
        local,
        mesh=mesh,
        in_specs=(P("batch", "feat"), P("batch", "feat")),
        out_specs=(P(), P("batch", "feat"), P("batch", "feat")),
        check_vma=False,
    )
```

```python
import functools

import jax
import jax.numpy as jnp
from jax import lax
from jax.experimental import pallas as pl
from jax.experimental.pallas import tpu as pltpu
from jax.sharding import PartitionSpec as P

MESH = pl.DeviceIdType.MESH
ROWS_T = (((1,), (1,)), ((), ()))

variance_floor = 0.25
redundancy = 0.0051


def plain(view_a, view_b):
    rows_dev, cols_dev = view_a.shape
    groups = lax.axis_size("batch")
    batch_total = rows_dev * groups
    feature_total = cols_dev * lax.axis_size("feat")
    scale = 2.0 * redundancy / batch_total
    all_a = lax.all_gather(view_a, "batch", axis=0, tiled=True).astype(jnp.float32)
    all_b = lax.all_gather(view_b, "batch", axis=0, tiled=True).astype(jnp.float32)

    def normalize(values):
        shifted = values - jnp.mean(values, axis=0)
        factor = lax.rsqrt(jnp.mean(shifted * shifted, axis=0) + variance_floor)
        return shifted * factor, factor

    full_a, factor_a = normalize(all_a)
    full_b, factor_b = normalize(all_b)
    samples_a = full_a.astype(jnp.bfloat16)
    samples_b = full_b.astype(jnp.bfloat16)
    start = lax.axis_index("batch") * rows_dev
    normed_a = lax.dynamic_slice_in_dim(full_a, start, rows_dev)
    normed_b = lax.dynamic_slice_in_dim(full_b, start, rows_dev)
    low_a = normed_a.astype(jnp.bfloat16)
    low_b = normed_b.astype(jnp.bfloat16)
    diagonal = (
        jnp.sum(samples_a.astype(jnp.float32) * samples_b.astype(jnp.float32), axis=0)
        / batch_total
    )
    rows_t = (((1,), (1,)), ((), ()))
    gram_a = lax.dot_general(low_a, samples_a, rows_t, preferred_element_type=jnp.float32)
    gram_b = lax.dot_general(low_b, samples_b, rows_t, preferred_element_type=jnp.float32)
    gram_a, gram_b = lax.psum((gram_a, gram_b), "feat")
    square_sum = jnp.sum(gram_a * gram_b) / (batch_total * batch_total)
    missing = 1.0 - diagonal
    on_diagonal = jnp.sum(missing * missing - redundancy * diagonal * diagonal)
    loss_value = (
        redundancy * lax.psum(square_sum, "batch") + lax.psum(on_diagonal, "feat")
    ) / feature_total
    ddiag = (2.0 * (diagonal - 1.0)).astype(jnp.bfloat16).astype(jnp.float32)
    rest = ddiag - 2.0 * redundancy * diagonal
    dnorm_a = scale * jnp.dot(
        gram_b.astype(jnp.bfloat16), samples_a, preferred_element_type=jnp.float32
    ) + low_b.astype(jnp.float32) * rest
    dnorm_b = scale * jnp.dot(
        gram_a.astype(jnp.bfloat16), samples_b, preferred_element_type=jnp.float32
    ) + low_a.astype(jnp.float32) * rest
    grad_totals = lax.psum(
        jnp.stack([
            jnp.sum(dnorm_a, axis=0),
            jnp.sum(dnorm_a * normed_a, axis=0),
            jnp.sum(dnorm_b, axis=0),
            jnp.sum(dnorm_b * normed_b, axis=0),
        ]),
        "batch",
    ) / batch_total
    grad_a = (dnorm_a - grad_totals[0] - normed_a * grad_totals[1]) * factor_a
    grad_b = (dnorm_b - grad_totals[2] - normed_b * grad_totals[3]) * factor_b
    return (loss_value, grad_a, grad_b)


def fold(values):
    rows, cols = values.shape
    return jnp.sum(values.reshape(rows // 8, 8, cols), axis=0)


def column_sums(rows, cols, count, term, step=16):
    zero = jnp.zeros((8, cols), jnp.float32)

    def body(i, carry):
        pieces = term(pl.ds(pl.multiple_of(i * step, step), step))
        return tuple(c + fold(p) for c, p in zip(carry, pieces))

    sums = lax.fori_loop(0, rows // step, body, (zero,) * count)
    return tuple(jnp.sum(s, axis=0, keepdims=True) for s in sums)


def kernel(
    feats, view_a, view_b, loss_ref, grad_a, grad_b,
    raw, low, part, pair_in, sum0, in0, sum1, in1, gram0, gram, rest0,
    stats, finals, losses,
    g_send, g_recv, s_send, s_recv, p_send, p_recv, z_send, z_recv,
    w_send, w_recv, q_send, q_recv, f_send, f_recv, l_send, l_recv,
):
    views, grads = (view_a, view_b), (grad_a, grad_b)
    rows, cols = view_a.shape
    half = rows // 2
    groups = 4
    depth = feats // 2
    share = half // depth
    samples = rows * groups
    features = cols * feats
    devices = groups * feats
    group, owner = lax.axis_index("batch"), lax.axis_index("feat")
    gy, gx = group // 2, group % 2
    peers = (gy * 2 + 1 - gx, (1 - gy) * 2 + gx, (1 - gy) * 2 + 1 - gx)
    z, core = owner // 2, owner % 2
    partner = z * 2 + 1 - core
    mine = pl.ds(pl.multiple_of(core * half, half), half)
    theirs = pl.ds(pl.multiple_of((1 - core) * half, half), half)
    me = group * feats + owner
    sent = []

    def send(src, dst, ssem, rsem, device):
        copy = pltpu.make_async_remote_copy(
            src_ref=src, dst_ref=dst, send_sem=ssem, recv_sem=rsem,
            device_id=device, device_id_type=MESH,
        )
        copy.start()
        sent.append(copy)
        return copy

    barrier = pltpu.get_barrier_semaphore()

    @pl.loop(1, devices)
    def _(k):
        other = (me + k) % devices
        pl.semaphore_signal(
            barrier, inc=1,
            device_id={"batch": other // feats, "feat": other % feats},
            device_id_type=MESH,
        )

    pl.semaphore_wait(barrier, devices - 1)

    lower, upper = pl.ds(0, half), pl.ds(half, half)
    moves = {}

    def own(v, link, part_of):
        index = link * 2 + part_of
        span = (lower, upper)[part_of]
        moves[v, link, part_of] = send(
            views[v].at[span], raw.at[v, link, span],
            g_send.at[v, index], g_recv.at[v, index], {"batch": peers[link]},
        )

    def forward(v):
        for link, part_of in ((0, 0), (1, 1)):
            moves[v, link, part_of].wait_recv()
            span = (lower, upper)[part_of]
            moves[v, 2, part_of] = send(
                raw.at[v, link, span], raw.at[v, 2, span],
                g_send.at[v, 4 + part_of], g_recv.at[v, 4 + part_of],
                {"batch": peers[1 - link]},
            )

    own(0, 0, 0)
    own(0, 1, 1)

    means = column_sums(
        rows, cols, 2,
        lambda r: tuple(x[r].astype(jnp.float32) for x in views),
    )
    means = tuple(m / rows for m in means)

    def squares(r):
        shifted = tuple(x[r].astype(jnp.float32) - m for x, m in zip(views, means))
        return tuple(s * s for s in shifted)

    spreads = column_sums(rows, cols, 2, squares)
    stats[0, 0:1] = means[0]
    stats[0, 1:2] = means[1]
    stats[0, 2:3] = spreads[0]
    stats[0, 3:4] = spreads[1]
    stat_moves = [
        send(stats.at[0], stats.at[k + 1], s_send.at[k], s_recv.at[k], {"batch": peers[k]})
        for k in range(3)
    ]
    own(0, 0, 1)
    own(0, 1, 0)
    for move in stat_moves:
        move.wait_recv()

    def merged(row):
        first = [stats[k, row : row + 1] for k in range(4)]
        return first, (first[0] + first[1]) + (first[2] + first[3])

    centers, factors = [], []
    for v in range(2):
        each, total = merged(v)
        center = total / groups
        gaps = [(e - center) * (e - center) for e in each]
        gap = (gaps[0] + gaps[1]) + (gaps[2] + gaps[3])
        variance = (merged(2 + v)[1] + rows * gap) / samples
        centers.append(center)
        factors.append(lax.rsqrt(variance + variance_floor))

    def normalize(v, slot):
        source = views[v] if slot == 0 else raw.at[v, slot - 1]

        @pl.loop(0, rows // 16)
        def _(i):
            r = pl.ds(pl.multiple_of(i * 16, 16), 16)
            values = source[r].astype(jnp.float32)
            low[v, slot, r] = ((values - centers[v]) * factors[v]).astype(jnp.bfloat16)

    ring = {}

    def buffers(v, slot):
        p = v * 4 + slot
        if slot == 0:
            return p, sum0.at[v], in0.at[v], gram0.at[v]
        return p, sum1.at[v, slot - 1], in1.at[v, slot - 1], gram.at[v, slot]

    def product(v, slot):
        p = v * 4 + slot
        part[p] = lax.dot_general(
            low[v, 0], low[v, slot], ROWS_T, preferred_element_type=jnp.float32
        )
        ring["pair", p] = send(
            part.at[p, theirs], pair_in.at[p], p_send.at[p], p_recv.at[p], {"feat": partner}
        )

    def scatter(v, slot):
        p, total, arrivals, _ = buffers(v, slot)
        ring["pair", p].wait_recv()
        total[...] = (part[p, mine] + pair_in[p]).astype(total.dtype)
        for k in range(1, depth):
            target = (z + k) % depth
            ring["sum", p, k] = send(
                total.at[pl.ds(pl.multiple_of(target * share, share), share)],
                arrivals.at[k - 1], z_send.at[p, k - 1], z_recv.at[p, k - 1],
                {"feat": target * 2 + core},
            )

    def collect(v, slot):
        p, total, arrivals, result = buffers(v, slot)
        value = total[pl.ds(pl.multiple_of(z * share, share), share)].astype(jnp.float32)
        for k in range(1, depth):
            ring["sum", p, k].wait_recv()
            value = value + arrivals[k - 1].astype(jnp.float32)
        span = pl.ds(pl.multiple_of(core * half + z * share, share), share)
        result[span] = value.astype(result.dtype)
        for k in range(1, depth):
            ring["all", p, k] = send(
                result.at[span], result.at[span], w_send.at[p, k - 1], w_recv.at[p, k - 1],
                {"feat": (z + k) % depth * 2 + core},
            )

    def swap(v, slot):
        p, _, _, result = buffers(v, slot)
        for k in range(1, depth):
            ring["all", p, k].wait_recv()
        ring["swap", p] = send(
            result.at[mine], result.at[mine], q_send.at[p], q_recv.at[p], {"feat": partner}
        )

    def finish(v, slot):
        ring["swap", v * 4 + slot].wait_recv()
        if slot == 0:
            high = gram0[v].astype(jnp.bfloat16)
            gram[v, 0] = high
            rest0[v] = (gram0[v] - high.astype(jnp.float32)).astype(jnp.bfloat16)

    forward(0)
    for link, part_of in ((0, 0), (1, 1), (0, 1), (1, 0)):
        own(1, link, part_of)
    normalize(0, 0)
    product(0, 0)
    normalize(1, 0)
    product(1, 0)
    scatter(0, 0)
    scatter(1, 0)
    moves[0, 0, 1].wait_recv()
    normalize(0, 1)
    product(0, 1)
    moves[0, 1, 0].wait_recv()
    normalize(0, 2)
    product(0, 2)
    collect(0, 0)
    collect(1, 0)
    scatter(0, 1)
    scatter(0, 2)
    swap(0, 0)
    swap(1, 0)
    moves[0, 2, 0].wait_recv()
    moves[0, 2, 1].wait_recv()
    normalize(0, 3)
    product(0, 3)
    collect(0, 1)
    collect(0, 2)
    scatter(0, 3)
    finish(0, 0)
    finish(1, 0)
    swap(0, 1)
    swap(0, 2)
    forward(1)
    collect(0, 3)
    finish(0, 1)
    finish(0, 2)
    moves[1, 0, 1].wait_recv()
    normalize(1, 1)
    product(1, 1)
    moves[1, 1, 0].wait_recv()
    normalize(1, 2)
    product(1, 2)
    swap(0, 3)
    scatter(1, 1)
    scatter(1, 2)
    collect(1, 1)
    collect(1, 2)
    finish(0, 3)
    swap(1, 1)
    swap(1, 2)
    moves[1, 2, 0].wait_recv()
    moves[1, 2, 1].wait_recv()
    normalize(1, 3)
    product(1, 3)
    scatter(1, 3)

    def term(slot):
        return lambda r: (
            low[0, slot, r].astype(jnp.float32) * low[1, slot, r].astype(jnp.float32),
        )

    diagonal = sum(column_sums(rows, cols, 1, term(slot))[0] for slot in range(4)) / samples
    missing = 1.0 - diagonal
    on_diagonal = jnp.sum(missing * missing - redundancy * diagonal * diagonal)
    ddiag = (2.0 * (diagonal - 1.0)).astype(jnp.bfloat16).astype(jnp.float32)
    rest = ddiag - 2.0 * redundancy * diagonal
    scale = 2.0 * redundancy / samples
    collect(1, 3)

    width = min(256, cols)

    def spread(v, slots, add):
        other = 1 - v

        @pl.loop(0, cols // width)
        def _(i):
            c = pl.ds(pl.multiple_of(i * width, width), width)
            if add:
                total = grads[other][:, c]
            else:
                total = jnp.dot(rest0[v], low[other, 0, :, c], preferred_element_type=jnp.float32)
            for slot in slots:
                total = total + jnp.dot(
                    gram[v, slot], low[other, slot, :, c], preferred_element_type=jnp.float32
                )
            grads[other][:, c] = total

    final_moves = {}

    def reduce_final(v):
        def body(r):
            dnorm = scale * grads[v][r] + low[1 - v, 0, r].astype(jnp.float32) * rest
            normed = (views[v][r].astype(jnp.float32) - centers[v]) * factors[v]
            grads[v][r] = dnorm
            return dnorm, dnorm * normed

        first, second = column_sums(rows, cols, 2, body)
        finals[v, 0, 0:1] = first
        finals[v, 0, 1:2] = second
        for k in range(3):
            final_moves[v, k] = send(
                finals.at[v, 0], finals.at[v, k + 1], f_send.at[v, k], f_recv.at[v, k],
                {"batch": peers[k]},
            )

    def write_final(v):
        for k in range(3):
            final_moves[v, k].wait_recv()
        first, second = (
            ((finals[v, 0, i : i + 1] + finals[v, 1, i : i + 1])
             + (finals[v, 2, i : i + 1] + finals[v, 3, i : i + 1])) / samples
            for i in range(2)
        )

        @pl.loop(0, rows // 16)
        def _(i):
            r = pl.ds(pl.multiple_of(i * 16, 16), 16)
            normed = (views[v][r].astype(jnp.float32) - centers[v]) * factors[v]
            grads[v][r] = (grads[v][r] - first - normed * second) * factors[v]

    finish(1, 1)
    finish(1, 2)
    spread(0, range(4), False)
    swap(1, 3)
    reduce_final(1)
    spread(1, range(3), False)
    finish(1, 3)
    spread(1, (3,), True)
    reduce_final(0)

    def gram_term(slot):
        def body(r):
            if slot == 0:
                return (gram0[0, r] * gram0[1, r],)
            return (gram[0, slot, r].astype(jnp.float32) * gram[1, slot, r].astype(jnp.float32),)

        return body

    square = sum(column_sums(rows, rows, 1, gram_term(slot))[0] for slot in range(4))
    square_sum = jnp.sum(square) / (samples * samples)
    share_of_loss = redundancy * square_sum / feats + on_diagonal / groups
    losses[me] = jnp.full((8, 128), share_of_loss, jnp.float32)

    def loss_copy(k):
        other = (me + k) % devices
        return pltpu.make_async_remote_copy(
            src_ref=losses.at[me], dst_ref=losses.at[me], send_sem=l_send, recv_sem=l_recv,
            device_id={"batch": other // feats, "feat": other % feats}, device_id_type=MESH,
        )

    @pl.loop(1, devices)
    def _(k):
        loss_copy(k).start()

    write_final(1)
    write_final(0)
    rest_of = losses.at[pl.ds(0, devices - 1)]
    pltpu.make_async_copy(rest_of, rest_of, l_recv).wait()
    loss_ref[...] = jnp.sum(losses[...], axis=0) / features
    pltpu.make_async_copy(rest_of, rest_of, l_send).wait()
    for copy in sent:
        copy.wait_send()


def local(feats, view_a, view_b):
    rows, cols = view_a.shape
    half, depth = rows // 2, feats // 2
    share = half // depth
    f32, bf16 = jnp.float32, jnp.bfloat16
    dma = pltpu.SemaphoreType.DMA
    vmem = pl.BlockSpec(memory_space=pltpu.VMEM)
    loss, grad_a, grad_b = pl.pallas_call(
        functools.partial(kernel, feats),
        out_shape=(
            jax.ShapeDtypeStruct((8, 128), f32),
            jax.ShapeDtypeStruct((rows, cols), f32),
            jax.ShapeDtypeStruct((rows, cols), f32),
        ),
        in_specs=[vmem, vmem],
        out_specs=(vmem, vmem, vmem),
        scratch_shapes=[
            pltpu.VMEM((2, 3, rows, cols), bf16),
            pltpu.VMEM((2, 4, rows, cols), bf16),
            pltpu.VMEM((8, rows, rows), f32),
            pltpu.VMEM((8, half, rows), f32),
            pltpu.VMEM((2, half, rows), f32),
            pltpu.VMEM((2, depth - 1, share, rows), f32),
            pltpu.VMEM((2, 3, half, rows), bf16),
            pltpu.VMEM((2, 3, depth - 1, share, rows), bf16),
            pltpu.VMEM((2, rows, rows), f32),
            pltpu.VMEM((2, 4, rows, rows), bf16),
            pltpu.VMEM((2, rows, rows), bf16),
            pltpu.VMEM((4, 4, cols), f32),
            pltpu.VMEM((2, 4, 2, cols), f32),
            pltpu.VMEM((4 * feats, 8, 128), f32),
            dma((2, 6)), dma((2, 6)), dma((3,)), dma((3,)),
            dma((8,)), dma((8,)), dma((8, depth - 1)), dma((8, depth - 1)),
            dma((8, depth - 1)), dma((8, depth - 1)), dma((8,)), dma((8,)),
            dma((2, 3)), dma((2, 3)), dma, dma,
        ],
        compiler_params=pltpu.CompilerParams(
            collective_id=0, has_side_effects=True, vmem_limit_bytes=56 * 1024 * 1024
        ),
        name="twins",
    )(view_a, view_b)
    return loss[0, 0], grad_a, grad_b


def solution(mesh):
    feats = mesh.shape["feat"]
    body = functools.partial(local, feats) if mesh.shape["batch"] == 4 else plain
    return jax.shard_map(
        body,
        mesh=mesh,
        in_specs=(P("batch", "feat"), P("batch", "feat")),
        out_specs=(P(), P("batch", "feat"), P("batch", "feat")),
        check_vma=False,
    )
```

```python
import functools

import jax
import jax.numpy as jnp
from jax import lax
from jax.experimental import pallas as pl
from jax.experimental.pallas import tpu as pltpu
from jax.sharding import PartitionSpec as P

MESH = pl.DeviceIdType.MESH
ROWS_T = (((1,), (1,)), ((), ()))

variance_floor = 0.25
redundancy = 0.0051


def plain(view_a, view_b):
    rows_dev, cols_dev = view_a.shape
    groups = lax.axis_size("batch")
    batch_total = rows_dev * groups
    feature_total = cols_dev * lax.axis_size("feat")
    scale = 2.0 * redundancy / batch_total
    all_a = lax.all_gather(view_a, "batch", axis=0, tiled=True).astype(jnp.float32)
    all_b = lax.all_gather(view_b, "batch", axis=0, tiled=True).astype(jnp.float32)

    def normalize(values):
        shifted = values - jnp.mean(values, axis=0)
        factor = lax.rsqrt(jnp.mean(shifted * shifted, axis=0) + variance_floor)
        return shifted * factor, factor

    full_a, factor_a = normalize(all_a)
    full_b, factor_b = normalize(all_b)
    samples_a = full_a.astype(jnp.bfloat16)
    samples_b = full_b.astype(jnp.bfloat16)
    start = lax.axis_index("batch") * rows_dev
    normed_a = lax.dynamic_slice_in_dim(full_a, start, rows_dev)
    normed_b = lax.dynamic_slice_in_dim(full_b, start, rows_dev)
    low_a = normed_a.astype(jnp.bfloat16)
    low_b = normed_b.astype(jnp.bfloat16)
    diagonal = (
        jnp.sum(samples_a.astype(jnp.float32) * samples_b.astype(jnp.float32), axis=0)
        / batch_total
    )
    rows_t = (((1,), (1,)), ((), ()))
    gram_a = lax.dot_general(low_a, samples_a, rows_t, preferred_element_type=jnp.float32)
    gram_b = lax.dot_general(low_b, samples_b, rows_t, preferred_element_type=jnp.float32)
    gram_a, gram_b = lax.psum((gram_a, gram_b), "feat")
    square_sum = jnp.sum(gram_a * gram_b) / (batch_total * batch_total)
    missing = 1.0 - diagonal
    on_diagonal = jnp.sum(missing * missing - redundancy * diagonal * diagonal)
    loss_value = (
        redundancy * lax.psum(square_sum, "batch") + lax.psum(on_diagonal, "feat")
    ) / feature_total
    ddiag = (2.0 * (diagonal - 1.0)).astype(jnp.bfloat16).astype(jnp.float32)
    rest = ddiag - 2.0 * redundancy * diagonal
    dnorm_a = scale * jnp.dot(
        gram_b.astype(jnp.bfloat16), samples_a, preferred_element_type=jnp.float32
    ) + low_b.astype(jnp.float32) * rest
    dnorm_b = scale * jnp.dot(
        gram_a.astype(jnp.bfloat16), samples_b, preferred_element_type=jnp.float32
    ) + low_a.astype(jnp.float32) * rest
    grad_totals = lax.psum(
        jnp.stack([
            jnp.sum(dnorm_a, axis=0),
            jnp.sum(dnorm_a * normed_a, axis=0),
            jnp.sum(dnorm_b, axis=0),
            jnp.sum(dnorm_b * normed_b, axis=0),
        ]),
        "batch",
    ) / batch_total
    grad_a = (dnorm_a - grad_totals[0] - normed_a * grad_totals[1]) * factor_a
    grad_b = (dnorm_b - grad_totals[2] - normed_b * grad_totals[3]) * factor_b
    return (loss_value, grad_a, grad_b)


def fold(values):
    rows, cols = values.shape
    return jnp.sum(values.reshape(rows // 8, 8, cols), axis=0)


def column_sums(rows, cols, count, term, step=16):
    zero = jnp.zeros((8, cols), jnp.float32)

    def body(i, carry):
        pieces = term(pl.ds(pl.multiple_of(i * step, step), step))
        return tuple(c + fold(p) for c, p in zip(carry, pieces))

    sums = lax.fori_loop(0, rows // step, body, (zero,) * count)
    return tuple(jnp.sum(s, axis=0, keepdims=True) for s in sums)


def kernel(
    feats, view_a, view_b, table, grad_a, grad_b,
    raw, low, part, pair_in, sum0, in0, sum1, in1, gram0, gram, rest0,
    stats, finals, losses,
    g_send, g_recv, s_send, s_recv, p_send, p_recv, z_send, z_recv,
    w_send, w_recv, q_send, q_recv, f_send, f_recv, l_send, l_recv,
):
    views, grads = (view_a, view_b), (grad_a, grad_b)
    rows, cols = view_a.shape
    half = rows // 2
    groups = 4
    depth = feats // 2
    share = half // depth
    samples = rows * groups
    features = cols * feats
    group, owner = lax.axis_index("batch"), lax.axis_index("feat")
    gy, gx = group // 2, group % 2
    peers = (gy * 2 + 1 - gx, (1 - gy) * 2 + gx, (1 - gy) * 2 + 1 - gx)
    z, core = owner // 2, owner % 2
    partner = z * 2 + 1 - core
    mine = pl.ds(pl.multiple_of(core * half, half), half)
    theirs = pl.ds(pl.multiple_of((1 - core) * half, half), half)
    sent = []

    def send(src, dst, ssem, rsem, device):
        copy = pltpu.make_async_remote_copy(
            src_ref=src, dst_ref=dst, send_sem=ssem, recv_sem=rsem,
            device_id=device, device_id_type=MESH,
        )
        copy.start()
        sent.append(copy)
        return copy

    barrier = pltpu.get_barrier_semaphore()

    for peer in peers:
        pl.semaphore_signal(barrier, inc=1, device_id={"batch": peer}, device_id_type=MESH)

    @pl.loop(1, feats)
    def _(k):
        pl.semaphore_signal(
            barrier, inc=1, device_id={"feat": (owner + k) % feats}, device_id_type=MESH
        )

    pl.semaphore_wait(barrier, len(peers) + feats - 1)

    lower, upper = pl.ds(0, half), pl.ds(half, half)
    moves = {}

    def own(v, link, part_of):
        index = link * 2 + part_of
        span = (lower, upper)[part_of]
        moves[v, link, part_of] = send(
            views[v].at[span], raw.at[v, link, span],
            g_send.at[v, index], g_recv.at[v, index], {"batch": peers[link]},
        )

    def forward(v):
        for link, part_of in ((0, 0), (1, 1)):
            moves[v, link, part_of].wait_recv()
            span = (lower, upper)[part_of]
            moves[v, 2, part_of] = send(
                raw.at[v, link, span], raw.at[v, 2, span],
                g_send.at[v, 4 + part_of], g_recv.at[v, 4 + part_of],
                {"batch": peers[1 - link]},
            )

    own(0, 0, 0)
    own(0, 1, 1)

    means = column_sums(
        rows, cols, 2,
        lambda r: tuple(x[r].astype(jnp.float32) for x in views),
    )
    means = tuple(m / rows for m in means)

    def squares(r):
        shifted = tuple(x[r].astype(jnp.float32) - m for x, m in zip(views, means))
        return tuple(s * s for s in shifted)

    spreads = column_sums(rows, cols, 2, squares)
    stats[0, 0:1] = means[0]
    stats[0, 1:2] = means[1]
    stats[0, 2:3] = spreads[0]
    stats[0, 3:4] = spreads[1]
    stat_moves = [
        send(stats.at[0], stats.at[k + 1], s_send.at[k], s_recv.at[k], {"batch": peers[k]})
        for k in range(3)
    ]
    own(0, 0, 1)
    own(0, 1, 0)
    for move in stat_moves:
        move.wait_recv()

    def merged(row):
        first = [stats[k, row : row + 1] for k in range(4)]
        return first, (first[0] + first[1]) + (first[2] + first[3])

    centers, factors = [], []
    for v in range(2):
        each, total = merged(v)
        center = total / groups
        gaps = [(e - center) * (e - center) for e in each]
        gap = (gaps[0] + gaps[1]) + (gaps[2] + gaps[3])
        variance = (merged(2 + v)[1] + rows * gap) / samples
        centers.append(center)
        factors.append(lax.rsqrt(variance + variance_floor))

    def normalize(v, slot, part_of=None):
        source = views[v] if slot == 0 else raw.at[v, slot - 1]
        count, base = (rows, 0) if part_of is None else (half, part_of * half)

        @pl.loop(0, count // 16)
        def _(i):
            r = pl.ds(pl.multiple_of(base + i * 16, 16), 16)
            values = source[r].astype(jnp.float32)
            low[v, slot, r] = ((values - centers[v]) * factors[v]).astype(jnp.bfloat16)

    ring = {}

    def buffers(v, slot):
        p = v * 4 + slot
        if slot == 0:
            return p, sum0.at[v], in0.at[v], gram0.at[v]
        return p, sum1.at[v, slot - 1], in1.at[v, slot - 1], gram.at[v, slot]

    def product(v, slot):
        p = v * 4 + slot
        part[p] = lax.dot_general(
            low[v, 0], low[v, slot], ROWS_T, preferred_element_type=jnp.float32
        )
        ring["pair", p] = send(
            part.at[p, theirs], pair_in.at[p], p_send.at[p], p_recv.at[p], {"feat": partner}
        )

    def scatter(v, slot):
        p, total, arrivals, _ = buffers(v, slot)
        ring["pair", p].wait_recv()
        total[...] = (part[p, mine] + pair_in[p]).astype(total.dtype)
        for k in range(1, depth):
            target = (z + k) % depth
            ring["sum", p, k] = send(
                total.at[pl.ds(pl.multiple_of(target * share, share), share)],
                arrivals.at[k - 1], z_send.at[p, k - 1], z_recv.at[p, k - 1],
                {"feat": target * 2 + core},
            )

    def collect(v, slot):
        p, total, arrivals, result = buffers(v, slot)
        value = total[pl.ds(pl.multiple_of(z * share, share), share)].astype(jnp.float32)
        for k in range(1, depth):
            ring["sum", p, k].wait_recv()
            value = value + arrivals[k - 1].astype(jnp.float32)
        span = pl.ds(pl.multiple_of(core * half + z * share, share), share)
        result[span] = value.astype(result.dtype)
        for k in range(1, depth):
            ring["all", p, k] = send(
                result.at[span], result.at[span], w_send.at[p, k - 1], w_recv.at[p, k - 1],
                {"feat": (z + k) % depth * 2 + core},
            )

    def swap(v, slot):
        p, _, _, result = buffers(v, slot)
        for k in range(1, depth):
            ring["all", p, k].wait_recv()
        ring["swap", p] = send(
            result.at[mine], result.at[mine], q_send.at[p], q_recv.at[p], {"feat": partner}
        )

    def finish(v, slot):
        ring["swap", v * 4 + slot].wait_recv()
        if slot == 0:
            high = gram0[v].astype(jnp.bfloat16)
            gram[v, 0] = high
            rest0[v] = (gram0[v] - high.astype(jnp.float32)).astype(jnp.bfloat16)

    def term(slot):
        return lambda r: (
            low[0, slot, r].astype(jnp.float32) * low[1, slot, r].astype(jnp.float32),
        )

    def diagonal_sum(slot):
        return column_sums(rows, cols, 1, term(slot))[0]

    width = min(256, cols)

    def spread(v, slots, add):
        other = 1 - v

        @pl.loop(0, cols // width)
        def _(i):
            c = pl.ds(pl.multiple_of(i * width, width), width)
            if add:
                total = grads[other][:, c]
            else:
                total = jnp.dot(rest0[v], low[other, 0, :, c], preferred_element_type=jnp.float32)
            for slot in slots:
                total = total + jnp.dot(
                    gram[v, slot], low[other, slot, :, c], preferred_element_type=jnp.float32
                )
            grads[other][:, c] = total

    def gram_product(slot):
        def body(r):
            if slot == 0:
                return (gram0[0, r] * gram0[1, r],)
            return (gram[0, slot, r].astype(jnp.float32) * gram[1, slot, r].astype(jnp.float32),)

        return column_sums(rows, rows, 1, body)[0]

    forward(0)
    for link, part_of in ((0, 0), (1, 1), (0, 1), (1, 0)):
        own(1, link, part_of)
    normalize(0, 0)
    product(0, 0)
    normalize(1, 0)
    product(1, 0)
    normalize(0, 1, 0)
    normalize(0, 2, 1)
    scatter(0, 0)
    scatter(1, 0)
    moves[0, 0, 1].wait_recv()
    normalize(0, 1, 1)
    product(0, 1)
    moves[0, 1, 0].wait_recv()
    normalize(0, 2, 0)
    product(0, 2)
    collect(0, 0)
    collect(1, 0)
    scatter(0, 1)
    scatter(0, 2)
    moves[0, 2, 0].wait_recv()
    moves[0, 2, 1].wait_recv()
    normalize(0, 3)
    product(0, 3)
    swap(0, 0)
    swap(1, 0)
    collect(0, 1)
    collect(0, 2)
    scatter(0, 3)
    finish(0, 0)
    finish(1, 0)
    forward(1)
    normalize(1, 1, 0)
    normalize(1, 2, 1)
    swap(0, 1)
    swap(0, 2)
    collect(0, 3)
    diagonal = diagonal_sum(0)
    square = gram_product(0)
    finish(0, 1)
    finish(0, 2)
    moves[1, 0, 1].wait_recv()
    normalize(1, 1, 1)
    product(1, 1)
    moves[1, 1, 0].wait_recv()
    normalize(1, 2, 0)
    product(1, 2)
    swap(0, 3)
    scatter(1, 1)
    scatter(1, 2)
    diagonal = diagonal + diagonal_sum(1) + diagonal_sum(2)
    finish(0, 3)
    spread(0, range(3), False)
    moves[1, 2, 0].wait_recv()
    moves[1, 2, 1].wait_recv()
    normalize(1, 3)
    product(1, 3)
    collect(1, 1)
    collect(1, 2)
    diagonal = (diagonal + diagonal_sum(3)) / samples
    missing = 1.0 - diagonal
    on_diagonal = jnp.sum(missing * missing - redundancy * diagonal * diagonal)
    scatter(1, 3)
    losses[owner] = jnp.full((8, 128), on_diagonal, jnp.float32)

    @pl.loop(1, feats)
    def _(k):
        pltpu.make_async_remote_copy(
            src_ref=losses.at[owner], dst_ref=losses.at[owner],
            send_sem=l_send, recv_sem=l_recv,
            device_id={"feat": (owner + k) % feats}, device_id_type=MESH,
        ).start()

    ddiag = (2.0 * (diagonal - 1.0)).astype(jnp.bfloat16).astype(jnp.float32)
    rest = ddiag - 2.0 * redundancy * diagonal
    scale = 2.0 * redundancy / samples
    final_moves = {}

    def reduce_final(v):
        def body(r):
            dnorm = scale * grads[v][r] + low[1 - v, 0, r].astype(jnp.float32) * rest
            normed = (views[v][r].astype(jnp.float32) - centers[v]) * factors[v]
            grads[v][r] = dnorm
            return dnorm, dnorm * normed

        first, second = column_sums(rows, cols, 2, body)
        finals[v, 0, 0:1] = first
        finals[v, 0, 1:2] = second

    def exchange_final(v):
        for k in range(3):
            final_moves[v, k] = send(
                finals.at[v, 0], finals.at[v, k + 1], f_send.at[v, k], f_recv.at[v, k],
                {"batch": peers[k]},
            )

    def merge_final(v, count):
        for k in range(3):
            final_moves[v, k].wait_recv()
        return tuple(
            (finals[v, 0, i : i + 1] + finals[v, 1, i : i + 1])
            + (finals[v, 2, i : i + 1] + finals[v, 3, i : i + 1])
            for i in range(count)
        )

    spread(0, (3,), True)
    collect(1, 3)
    swap(1, 1)
    swap(1, 2)
    reduce_final(1)
    exchange_final(1)
    finish(1, 1)
    finish(1, 2)
    spread(1, range(3), False)
    swap(1, 3)
    square = square + gram_product(1) + gram_product(2)
    rest_of = losses.at[pl.ds(0, feats - 1)]
    pltpu.make_async_copy(rest_of, rest_of, l_recv).wait()
    on_diagonal_all = jnp.sum(losses[...], axis=0)[0:1, 0:1]
    finish(1, 3)
    spread(1, (3,), True)
    reduce_final(0)
    square = square + gram_product(3)
    loss_part = redundancy * jnp.sum(square) / (samples * samples) + on_diagonal_all / groups
    finals[0, 0, 2:3] = jnp.broadcast_to(loss_part, (1, cols))
    exchange_final(0)
    for v in (1, 0):
        table[4 * v : 4 * v + 1] = centers[v]
        table[4 * v + 1 : 4 * v + 2] = factors[v]
    pltpu.make_async_copy(rest_of, rest_of, l_send).wait()
    for v in (1, 0):
        sums = merge_final(v, 3 - v)
        table[4 * v + 2 : 4 * v + 3] = sums[0] / samples
        table[4 * v + 3 : 4 * v + 4] = sums[1] / samples
        if v == 0:
            table[8:9] = sums[2] / features
    for copy in sent:
        copy.wait_send()


def local(feats, view_a, view_b):
    rows, cols = view_a.shape
    half, depth = rows // 2, feats // 2
    share = half // depth
    f32, bf16 = jnp.float32, jnp.bfloat16
    dma = pltpu.SemaphoreType.DMA
    vmem = pl.BlockSpec(memory_space=pltpu.VMEM)
    table, dnorm_a, dnorm_b = pl.pallas_call(
        functools.partial(kernel, feats),
        out_shape=(
            jax.ShapeDtypeStruct((16, cols), f32),
            jax.ShapeDtypeStruct((rows, cols), f32),
            jax.ShapeDtypeStruct((rows, cols), f32),
        ),
        in_specs=[vmem, vmem],
        out_specs=(vmem, vmem, vmem),
        scratch_shapes=[
            pltpu.VMEM((2, 3, rows, cols), bf16),
            pltpu.VMEM((2, 4, rows, cols), bf16),
            pltpu.VMEM((8, rows, rows), f32),
            pltpu.VMEM((8, half, rows), f32),
            pltpu.VMEM((2, half, rows), f32),
            pltpu.VMEM((2, depth - 1, share, rows), f32),
            pltpu.VMEM((2, 3, half, rows), bf16),
            pltpu.VMEM((2, 3, depth - 1, share, rows), bf16),
            pltpu.VMEM((2, rows, rows), f32),
            pltpu.VMEM((2, 4, rows, rows), bf16),
            pltpu.VMEM((2, rows, rows), bf16),
            pltpu.VMEM((4, 4, cols), f32),
            pltpu.VMEM((2, 4, 4, cols), f32),
            pltpu.VMEM((feats, 8, 128), f32),
            dma((2, 6)), dma((2, 6)), dma((3,)), dma((3,)),
            dma((8,)), dma((8,)), dma((8, depth - 1)), dma((8, depth - 1)),
            dma((8, depth - 1)), dma((8, depth - 1)), dma((8,)), dma((8,)),
            dma((2, 3)), dma((2, 3)), dma, dma,
        ],
        compiler_params=pltpu.CompilerParams(
            collective_id=0, has_side_effects=True, vmem_limit_bytes=56 * 1024 * 1024
        ),
        name="twins",
    )(view_a, view_b)

    def grad(dnorm, view, at):
        center, factor, first, second = (table[at + i] for i in range(4))
        normed = (view.astype(f32) - center) * factor
        return (dnorm - first - normed * second) * factor

    return table[8, 0], grad(dnorm_a, view_a, 0), grad(dnorm_b, view_b, 4)


def solution(mesh):
    feats = mesh.shape["feat"]
    body = functools.partial(local, feats) if mesh.shape["batch"] == 4 else plain
    return jax.shard_map(
        body,
        mesh=mesh,
        in_specs=(P("batch", "feat"), P("batch", "feat")),
        out_specs=(P(), P("batch", "feat"), P("batch", "feat")),
        check_vma=False,
    )
```

```python
import functools

import jax
import jax.numpy as jnp
from jax import lax
from jax.experimental import pallas as pl
from jax.experimental.pallas import tpu as pltpu
from jax.sharding import PartitionSpec as P

MESH = pl.DeviceIdType.MESH
ROWS_T = (((1,), (1,)), ((), ()))

variance_floor = 0.25
redundancy = 0.0051


def plain(view_a, view_b):
    rows_dev, cols_dev = view_a.shape
    groups = lax.axis_size("batch")
    batch_total = rows_dev * groups
    feature_total = cols_dev * lax.axis_size("feat")
    scale = 2.0 * redundancy / batch_total
    all_a = lax.all_gather(view_a, "batch", axis=0, tiled=True).astype(jnp.float32)
    all_b = lax.all_gather(view_b, "batch", axis=0, tiled=True).astype(jnp.float32)

    def normalize(values):
        shifted = values - jnp.mean(values, axis=0)
        factor = lax.rsqrt(jnp.mean(shifted * shifted, axis=0) + variance_floor)
        return shifted * factor, factor

    full_a, factor_a = normalize(all_a)
    full_b, factor_b = normalize(all_b)
    samples_a = full_a.astype(jnp.bfloat16)
    samples_b = full_b.astype(jnp.bfloat16)
    start = lax.axis_index("batch") * rows_dev
    normed_a = lax.dynamic_slice_in_dim(full_a, start, rows_dev)
    normed_b = lax.dynamic_slice_in_dim(full_b, start, rows_dev)
    low_a = normed_a.astype(jnp.bfloat16)
    low_b = normed_b.astype(jnp.bfloat16)
    diagonal = (
        jnp.sum(samples_a.astype(jnp.float32) * samples_b.astype(jnp.float32), axis=0)
        / batch_total
    )
    rows_t = (((1,), (1,)), ((), ()))
    gram_a = lax.dot_general(low_a, samples_a, rows_t, preferred_element_type=jnp.float32)
    gram_b = lax.dot_general(low_b, samples_b, rows_t, preferred_element_type=jnp.float32)
    gram_a, gram_b = lax.psum((gram_a, gram_b), "feat")
    square_sum = jnp.sum(gram_a * gram_b) / (batch_total * batch_total)
    missing = 1.0 - diagonal
    on_diagonal = jnp.sum(missing * missing - redundancy * diagonal * diagonal)
    loss_value = (
        redundancy * lax.psum(square_sum, "batch") + lax.psum(on_diagonal, "feat")
    ) / feature_total
    ddiag = (2.0 * (diagonal - 1.0)).astype(jnp.bfloat16).astype(jnp.float32)
    rest = ddiag - 2.0 * redundancy * diagonal
    dnorm_a = scale * jnp.dot(
        gram_b.astype(jnp.bfloat16), samples_a, preferred_element_type=jnp.float32
    ) + low_b.astype(jnp.float32) * rest
    dnorm_b = scale * jnp.dot(
        gram_a.astype(jnp.bfloat16), samples_b, preferred_element_type=jnp.float32
    ) + low_a.astype(jnp.float32) * rest
    grad_totals = lax.psum(
        jnp.stack([
            jnp.sum(dnorm_a, axis=0),
            jnp.sum(dnorm_a * normed_a, axis=0),
            jnp.sum(dnorm_b, axis=0),
            jnp.sum(dnorm_b * normed_b, axis=0),
        ]),
        "batch",
    ) / batch_total
    grad_a = (dnorm_a - grad_totals[0] - normed_a * grad_totals[1]) * factor_a
    grad_b = (dnorm_b - grad_totals[2] - normed_b * grad_totals[3]) * factor_b
    return (loss_value, grad_a, grad_b)


def fold(values):
    rows, cols = values.shape
    return jnp.sum(values.reshape(rows // 8, 8, cols), axis=0)


def column_sums(rows, cols, count, term, step=16):
    zero = jnp.zeros((8, cols), jnp.float32)

    def body(i, carry):
        pieces = term(pl.ds(pl.multiple_of(i * step, step), step))
        return tuple(c + fold(p) for c, p in zip(carry, pieces))

    sums = lax.fori_loop(0, rows // step, body, (zero,) * count)
    return tuple(jnp.sum(s, axis=0, keepdims=True) for s in sums)


def kernel(
    feats, view_a, view_b, table, grad_a, grad_b,
    raw, low, part, pair_in, sum0, in0, sum1, in1, gram0, gram, rest0,
    stats, finals, losses,
    g_send, g_recv, s_send, s_recv, p_send, p_recv, z_send, z_recv,
    w_send, w_recv, q_send, q_recv, f_send, f_recv, l_send, l_recv,
):
    views, grads = (view_a, view_b), (grad_a, grad_b)
    rows, cols = view_a.shape
    half = rows // 2
    groups = 4
    depth = feats // 2
    share = half // depth
    samples = rows * groups
    features = cols * feats
    group, owner = lax.axis_index("batch"), lax.axis_index("feat")
    gy, gx = group // 2, group % 2
    peers = (gy * 2 + 1 - gx, (1 - gy) * 2 + gx, (1 - gy) * 2 + 1 - gx)
    z, core = owner // 2, owner % 2
    partner = z * 2 + 1 - core
    mine = pl.ds(pl.multiple_of(core * half, half), half)
    theirs = pl.ds(pl.multiple_of((1 - core) * half, half), half)
    sent = []

    def send(src, dst, ssem, rsem, device):
        copy = pltpu.make_async_remote_copy(
            src_ref=src, dst_ref=dst, send_sem=ssem, recv_sem=rsem,
            device_id=device, device_id_type=MESH,
        )
        copy.start()
        sent.append(copy)
        return copy

    barrier = pltpu.get_barrier_semaphore()

    for peer in peers:
        pl.semaphore_signal(barrier, inc=1, device_id={"batch": peer}, device_id_type=MESH)

    @pl.loop(1, feats)
    def _(k):
        pl.semaphore_signal(
            barrier, inc=1, device_id={"feat": (owner + k) % feats}, device_id_type=MESH
        )

    pl.semaphore_wait(barrier, len(peers) + feats - 1)

    lower, upper = pl.ds(0, half), pl.ds(half, half)
    moves = {}

    def own(v, link, part_of):
        index = link * 2 + part_of
        span = (lower, upper)[part_of]
        moves[v, link, part_of] = send(
            views[v].at[span], raw.at[v, link, span],
            g_send.at[v, index], g_recv.at[v, index], {"batch": peers[link]},
        )

    def forward(v):
        for link, part_of in ((0, 0), (1, 1)):
            moves[v, link, part_of].wait_recv()
            span = (lower, upper)[part_of]
            moves[v, 2, part_of] = send(
                raw.at[v, link, span], raw.at[v, 2, span],
                g_send.at[v, 4 + part_of], g_recv.at[v, 4 + part_of],
                {"batch": peers[1 - link]},
            )

    own(0, 0, 0)
    own(0, 1, 1)

    means = column_sums(
        rows, cols, 2,
        lambda r: tuple(x[r].astype(jnp.float32) for x in views),
    )
    means = tuple(m / rows for m in means)

    def squares(r):
        shifted = tuple(x[r].astype(jnp.float32) - m for x, m in zip(views, means))
        return tuple(s * s for s in shifted)

    spreads = column_sums(rows, cols, 2, squares)
    stats[0, 0:1] = means[0]
    stats[0, 1:2] = means[1]
    stats[0, 2:3] = spreads[0]
    stats[0, 3:4] = spreads[1]
    stat_moves = [
        send(stats.at[0], stats.at[k + 1], s_send.at[k], s_recv.at[k], {"batch": peers[k]})
        for k in range(3)
    ]
    own(0, 0, 1)
    own(0, 1, 0)
    for move in stat_moves:
        move.wait_recv()

    def merged(row):
        first = [stats[k, row : row + 1] for k in range(4)]
        return first, (first[0] + first[1]) + (first[2] + first[3])

    centers, factors = [], []
    for v in range(2):
        each, total = merged(v)
        center = total / groups
        gaps = [(e - center) * (e - center) for e in each]
        gap = (gaps[0] + gaps[1]) + (gaps[2] + gaps[3])
        variance = (merged(2 + v)[1] + rows * gap) / samples
        centers.append(center)
        factors.append(lax.rsqrt(variance + variance_floor))

    def normalize(v, slot, part_of=None):
        source = views[v] if slot == 0 else raw.at[v, slot - 1]
        count, base = (rows, 0) if part_of is None else (half, part_of * half)

        @pl.loop(0, count // 16)
        def _(i):
            r = pl.ds(pl.multiple_of(base + i * 16, 16), 16)
            values = source[r].astype(jnp.float32)
            low[v, slot, r] = ((values - centers[v]) * factors[v]).astype(jnp.bfloat16)

    ring = {}

    def buffers(v, slot):
        p = v * 4 + slot
        if slot == 0:
            return p, sum0.at[v], in0.at[v], gram0.at[v]
        return p, sum1.at[v, slot - 1], in1.at[v, slot - 1], gram.at[v, slot]

    def product(v, slot):
        p = v * 4 + slot
        part[p] = lax.dot_general(
            low[v, 0], low[v, slot], ROWS_T, preferred_element_type=jnp.float32
        )
        ring["pair", p] = send(
            part.at[p, theirs], pair_in.at[p], p_send.at[p], p_recv.at[p], {"feat": partner}
        )

    def scatter(v, slot):
        p, total, arrivals, _ = buffers(v, slot)
        ring["pair", p].wait_recv()
        total[...] = (part[p, mine] + pair_in[p]).astype(total.dtype)
        for k in range(1, depth):
            target = (z + k) % depth
            ring["sum", p, k] = send(
                total.at[pl.ds(pl.multiple_of(target * share, share), share)],
                arrivals.at[k - 1], z_send.at[p, k - 1], z_recv.at[p, k - 1],
                {"feat": target * 2 + core},
            )

    def collect(v, slot):
        p, total, arrivals, result = buffers(v, slot)
        value = total[pl.ds(pl.multiple_of(z * share, share), share)].astype(jnp.float32)
        for k in range(1, depth):
            ring["sum", p, k].wait_recv()
            value = value + arrivals[k - 1].astype(jnp.float32)
        span = pl.ds(pl.multiple_of(core * half + z * share, share), share)
        result[span] = value.astype(result.dtype)
        for k in range(1, depth):
            ring["all", p, k] = send(
                result.at[span], result.at[span], w_send.at[p, k - 1], w_recv.at[p, k - 1],
                {"feat": (z + k) % depth * 2 + core},
            )

    def swap(v, slot):
        p, _, _, result = buffers(v, slot)
        for k in range(1, depth):
            ring["all", p, k].wait_recv()
        ring["swap", p] = send(
            result.at[mine], result.at[mine], q_send.at[p], q_recv.at[p], {"feat": partner}
        )

    def finish(v, slot):
        ring["swap", v * 4 + slot].wait_recv()
        if slot == 0:
            high = gram0[v].astype(jnp.bfloat16)
            gram[v, 0] = high
            rest0[v] = (gram0[v] - high.astype(jnp.float32)).astype(jnp.bfloat16)

    def term(slot):
        return lambda r: (
            low[0, slot, r].astype(jnp.float32) * low[1, slot, r].astype(jnp.float32),
        )

    def diagonal_sum(slot):
        return column_sums(rows, cols, 1, term(slot))[0]

    width = min(256, cols)

    def spread(v, slots, add):
        other = 1 - v

        @pl.loop(0, cols // width)
        def _(i):
            c = pl.ds(pl.multiple_of(i * width, width), width)
            if add:
                total = grads[other][:, c]
            else:
                total = jnp.dot(rest0[v], low[other, 0, :, c], preferred_element_type=jnp.float32)
            for slot in slots:
                total = total + jnp.dot(
                    gram[v, slot], low[other, slot, :, c], preferred_element_type=jnp.float32
                )
            grads[other][:, c] = total

    def gram_product(slot):
        def body(r):
            if slot == 0:
                return (gram0[0, r] * gram0[1, r],)
            return (gram[0, slot, r].astype(jnp.float32) * gram[1, slot, r].astype(jnp.float32),)

        return column_sums(rows, rows, 1, body)[0]

    forward(0)
    for link, part_of in ((0, 0), (1, 1), (0, 1), (1, 0)):
        own(1, link, part_of)
    normalize(0, 0)
    product(0, 0)
    normalize(1, 0)
    product(1, 0)
    normalize(0, 1, 0)
    normalize(0, 2, 1)
    scatter(0, 0)
    scatter(1, 0)
    moves[0, 0, 1].wait_recv()
    normalize(0, 1, 1)
    product(0, 1)
    moves[0, 1, 0].wait_recv()
    normalize(0, 2, 0)
    product(0, 2)
    collect(0, 0)
    collect(1, 0)
    scatter(0, 1)
    scatter(0, 2)
    moves[0, 2, 0].wait_recv()
    moves[0, 2, 1].wait_recv()
    normalize(0, 3)
    product(0, 3)
    swap(0, 0)
    swap(1, 0)
    collect(0, 1)
    collect(0, 2)
    scatter(0, 3)
    finish(0, 0)
    finish(1, 0)
    forward(1)
    normalize(1, 1, 0)
    normalize(1, 2, 1)
    swap(0, 1)
    swap(0, 2)
    collect(0, 3)
    diagonal = diagonal_sum(0)
    square = gram_product(0)
    finish(0, 1)
    finish(0, 2)
    moves[1, 0, 1].wait_recv()
    normalize(1, 1, 1)
    product(1, 1)
    moves[1, 1, 0].wait_recv()
    normalize(1, 2, 0)
    product(1, 2)
    swap(0, 3)
    scatter(1, 1)
    scatter(1, 2)
    diagonal = diagonal + diagonal_sum(1) + diagonal_sum(2)
    finish(0, 3)
    spread(0, range(3), False)
    moves[1, 2, 0].wait_recv()
    moves[1, 2, 1].wait_recv()
    normalize(1, 3)
    product(1, 3)
    collect(1, 1)
    collect(1, 2)
    diagonal = (diagonal + diagonal_sum(3)) / samples
    missing = 1.0 - diagonal
    on_diagonal = jnp.sum(missing * missing - redundancy * diagonal * diagonal)
    scatter(1, 3)
    losses[owner] = jnp.full((8, 128), on_diagonal, jnp.float32)

    @pl.loop(1, feats)
    def _(k):
        pltpu.make_async_remote_copy(
            src_ref=losses.at[owner], dst_ref=losses.at[owner],
            send_sem=l_send, recv_sem=l_recv,
            device_id={"feat": (owner + k) % feats}, device_id_type=MESH,
        ).start()

    ddiag = (2.0 * (diagonal - 1.0)).astype(jnp.bfloat16).astype(jnp.float32)
    rest = ddiag - 2.0 * redundancy * diagonal
    scale = 2.0 * redundancy / samples
    final_moves = {}

    def reduce_final(v):
        def body(r):
            dnorm = scale * grads[v][r] + low[1 - v, 0, r].astype(jnp.float32) * rest
            normed = (views[v][r].astype(jnp.float32) - centers[v]) * factors[v]
            grads[v][r] = dnorm
            return dnorm, dnorm * normed

        first, second = column_sums(rows, cols, 2, body)
        finals[v, 0, 0:1] = first
        finals[v, 0, 1:2] = second

    def exchange_final(v):
        for k in range(3):
            final_moves[v, k] = send(
                finals.at[v, 0], finals.at[v, k + 1], f_send.at[v, k], f_recv.at[v, k],
                {"batch": peers[k]},
            )

    def merge_final(v, count):
        for k in range(3):
            final_moves[v, k].wait_recv()
        return tuple(
            (finals[v, 0, i : i + 1] + finals[v, 1, i : i + 1])
            + (finals[v, 2, i : i + 1] + finals[v, 3, i : i + 1])
            for i in range(count)
        )

    spread(0, (3,), True)
    collect(1, 3)
    swap(1, 1)
    swap(1, 2)
    reduce_final(1)
    exchange_final(1)
    finish(1, 1)
    finish(1, 2)
    spread(1, range(3), False)
    swap(1, 3)
    square = square + gram_product(1) + gram_product(2)
    rest_of = losses.at[pl.ds(0, feats - 1)]
    pltpu.make_async_copy(rest_of, rest_of, l_recv).wait()
    on_diagonal_all = jnp.sum(losses[...], axis=0)[0:1, 0:1]
    finish(1, 3)
    spread(1, (3,), True)
    reduce_final(0)
    square = square + gram_product(3)
    loss_part = redundancy * jnp.sum(square) / (samples * samples) + on_diagonal_all / groups
    finals[0, 0, 2:3] = jnp.broadcast_to(loss_part, (1, cols))
    exchange_final(0)
    for v in (1, 0):
        table[4 * v : 4 * v + 1] = centers[v]
        table[4 * v + 1 : 4 * v + 2] = factors[v]
    pltpu.make_async_copy(rest_of, rest_of, l_send).wait()
    for v in (1, 0):
        sums = merge_final(v, 3 - v)
        table[4 * v + 2 : 4 * v + 3] = sums[0] / samples
        table[4 * v + 3 : 4 * v + 4] = sums[1] / samples
        if v == 0:
            table[8:9] = sums[2] / features
    for copy in sent:
        copy.wait_send()


def last_step(table, dnorm_a, dnorm_b, view_a, view_b, loss, grad_a, grad_b):
    rows = view_a.shape[0]
    for v, (dnorm, view, grad) in enumerate(((dnorm_a, view_a, grad_a), (dnorm_b, view_b, grad_b))):
        center, factor, first, second = (table[4 * v + i : 4 * v + i + 1] for i in range(4))

        @pl.loop(0, rows // 16)
        def _(i):
            r = pl.ds(pl.multiple_of(i * 16, 16), 16)
            normed = (view[r].astype(jnp.float32) - center) * factor
            grad[r] = (dnorm[r] - first - normed * second) * factor

    loss[...] = table[8:9, 0:1]


def local(feats, view_a, view_b):
    rows, cols = view_a.shape
    half, depth = rows // 2, feats // 2
    share = half // depth
    f32, bf16 = jnp.float32, jnp.bfloat16
    dma = pltpu.SemaphoreType.DMA
    vmem = pl.BlockSpec(memory_space=pltpu.VMEM)
    table, dnorm_a, dnorm_b = pl.pallas_call(
        functools.partial(kernel, feats),
        out_shape=(
            jax.ShapeDtypeStruct((16, cols), f32),
            jax.ShapeDtypeStruct((rows, cols), f32),
            jax.ShapeDtypeStruct((rows, cols), f32),
        ),
        in_specs=[vmem, vmem],
        out_specs=(vmem, vmem, vmem),
        scratch_shapes=[
            pltpu.VMEM((2, 3, rows, cols), bf16),
            pltpu.VMEM((2, 4, rows, cols), bf16),
            pltpu.VMEM((8, rows, rows), f32),
            pltpu.VMEM((8, half, rows), f32),
            pltpu.VMEM((2, half, rows), f32),
            pltpu.VMEM((2, depth - 1, share, rows), f32),
            pltpu.VMEM((2, 3, half, rows), bf16),
            pltpu.VMEM((2, 3, depth - 1, share, rows), bf16),
            pltpu.VMEM((2, rows, rows), f32),
            pltpu.VMEM((2, 4, rows, rows), bf16),
            pltpu.VMEM((2, rows, rows), bf16),
            pltpu.VMEM((4, 4, cols), f32),
            pltpu.VMEM((2, 4, 4, cols), f32),
            pltpu.VMEM((feats, 8, 128), f32),
            dma((2, 6)), dma((2, 6)), dma((3,)), dma((3,)),
            dma((8,)), dma((8,)), dma((8, depth - 1)), dma((8, depth - 1)),
            dma((8, depth - 1)), dma((8, depth - 1)), dma((8,)), dma((8,)),
            dma((2, 3)), dma((2, 3)), dma, dma,
        ],
        compiler_params=pltpu.CompilerParams(
            collective_id=0, has_side_effects=True, vmem_limit_bytes=20 * 1024 * 1024
        ),
        name="twins",
    )(view_a, view_b)

    loss, grad_a, grad_b = pl.pallas_call(
        last_step,
        out_shape=(
            jax.ShapeDtypeStruct((1, 1), f32),
            jax.ShapeDtypeStruct((rows, cols), f32),
            jax.ShapeDtypeStruct((rows, cols), f32),
        ),
        in_specs=[vmem] * 5,
        out_specs=(vmem, vmem, vmem),
        compiler_params=pltpu.CompilerParams(vmem_limit_bytes=16 * 1024 * 1024),
        name="last_step",
    )(table, dnorm_a, dnorm_b, view_a, view_b)
    return loss[0, 0], grad_a, grad_b


def solution(mesh):
    feats = mesh.shape["feat"]
    body = functools.partial(local, feats) if mesh.shape["batch"] == 4 else plain
    return jax.shard_map(
        body,
        mesh=mesh,
        in_specs=(P("batch", "feat"), P("batch", "feat")),
        out_specs=(P(), P("batch", "feat"), P("batch", "feat")),
        check_vma=False,
    )
```

```python
import functools

import jax
import jax.numpy as jnp
from jax import lax
from jax.experimental import pallas as pl
from jax.experimental.pallas import tpu as pltpu
from jax.sharding import PartitionSpec as P

MESH = pl.DeviceIdType.MESH
ROWS_T = (((1,), (1,)), ((), ()))

variance_floor = 0.25
redundancy = 0.0051


def plain(view_a, view_b):
    rows_dev, cols_dev = view_a.shape
    groups = lax.axis_size("batch")
    batch_total = rows_dev * groups
    feature_total = cols_dev * lax.axis_size("feat")
    scale = 2.0 * redundancy / batch_total
    all_a = lax.all_gather(view_a, "batch", axis=0, tiled=True).astype(jnp.float32)
    all_b = lax.all_gather(view_b, "batch", axis=0, tiled=True).astype(jnp.float32)

    def normalize(values):
        shifted = values - jnp.mean(values, axis=0)
        factor = lax.rsqrt(jnp.mean(shifted * shifted, axis=0) + variance_floor)
        return shifted * factor, factor

    full_a, factor_a = normalize(all_a)
    full_b, factor_b = normalize(all_b)
    samples_a = full_a.astype(jnp.bfloat16)
    samples_b = full_b.astype(jnp.bfloat16)
    start = lax.axis_index("batch") * rows_dev
    normed_a = lax.dynamic_slice_in_dim(full_a, start, rows_dev)
    normed_b = lax.dynamic_slice_in_dim(full_b, start, rows_dev)
    low_a = normed_a.astype(jnp.bfloat16)
    low_b = normed_b.astype(jnp.bfloat16)
    diagonal = (
        jnp.sum(samples_a.astype(jnp.float32) * samples_b.astype(jnp.float32), axis=0)
        / batch_total
    )
    rows_t = (((1,), (1,)), ((), ()))
    gram_a = lax.dot_general(low_a, samples_a, rows_t, preferred_element_type=jnp.float32)
    gram_b = lax.dot_general(low_b, samples_b, rows_t, preferred_element_type=jnp.float32)
    gram_a, gram_b = lax.psum((gram_a, gram_b), "feat")
    square_sum = jnp.sum(gram_a * gram_b) / (batch_total * batch_total)
    missing = 1.0 - diagonal
    on_diagonal = jnp.sum(missing * missing - redundancy * diagonal * diagonal)
    loss_value = (
        redundancy * lax.psum(square_sum, "batch") + lax.psum(on_diagonal, "feat")
    ) / feature_total
    ddiag = (2.0 * (diagonal - 1.0)).astype(jnp.bfloat16).astype(jnp.float32)
    rest = ddiag - 2.0 * redundancy * diagonal
    dnorm_a = scale * jnp.dot(
        gram_b.astype(jnp.bfloat16), samples_a, preferred_element_type=jnp.float32
    ) + low_b.astype(jnp.float32) * rest
    dnorm_b = scale * jnp.dot(
        gram_a.astype(jnp.bfloat16), samples_b, preferred_element_type=jnp.float32
    ) + low_a.astype(jnp.float32) * rest
    grad_totals = lax.psum(
        jnp.stack([
            jnp.sum(dnorm_a, axis=0),
            jnp.sum(dnorm_a * normed_a, axis=0),
            jnp.sum(dnorm_b, axis=0),
            jnp.sum(dnorm_b * normed_b, axis=0),
        ]),
        "batch",
    ) / batch_total
    grad_a = (dnorm_a - grad_totals[0] - normed_a * grad_totals[1]) * factor_a
    grad_b = (dnorm_b - grad_totals[2] - normed_b * grad_totals[3]) * factor_b
    return (loss_value, grad_a, grad_b)


def fold(values):
    rows, cols = values.shape
    return jnp.sum(values.reshape(rows // 8, 8, cols), axis=0)


def column_sums(rows, cols, count, term, step=16):
    zero = jnp.zeros((8, cols), jnp.float32)

    def body(i, carry):
        pieces = term(pl.ds(pl.multiple_of(i * step, step), step))
        return tuple(c + fold(p) for c, p in zip(carry, pieces))

    sums = lax.fori_loop(0, rows // step, body, (zero,) * count, unroll=4)
    return tuple(jnp.sum(s, axis=0, keepdims=True) for s in sums)


def kernel(
    feats, source_a, source_b, table, grad_a, grad_b, view_a, view_b, load,
    raw, low, part, pair_in, sum0, in0, sum1, in1, gram0, gram, rest0,
    stats, finals, losses,
    g_send, g_recv, s_send, s_recv, p_send, p_recv, z_send, z_recv,
    w_send, w_recv, q_send, q_recv, f_send, f_recv, l_send, l_recv,
):
    views, grads = (view_a, view_b), (grad_a, grad_b)
    rows, cols = view_a.shape
    loads = [
        pltpu.make_async_copy(source_a, view_a, load.at[0]),
        pltpu.make_async_copy(source_b, view_b, load.at[1]),
    ]
    for copy in loads:
        copy.start()
    half = rows // 2
    groups = 4
    depth = feats // 2
    share = half // depth
    samples = rows * groups
    features = cols * feats
    group, owner = lax.axis_index("batch"), lax.axis_index("feat")
    gy, gx = group // 2, group % 2
    peers = (gy * 2 + 1 - gx, (1 - gy) * 2 + gx, (1 - gy) * 2 + 1 - gx)
    z, core = owner // 2, owner % 2
    partner = z * 2 + 1 - core
    mine = pl.ds(pl.multiple_of(core * half, half), half)
    theirs = pl.ds(pl.multiple_of((1 - core) * half, half), half)
    sent = []

    def send(src, dst, ssem, rsem, device):
        copy = pltpu.make_async_remote_copy(
            src_ref=src, dst_ref=dst, send_sem=ssem, recv_sem=rsem,
            device_id=device, device_id_type=MESH,
        )
        copy.start()
        sent.append(copy)
        return copy

    barrier = pltpu.get_barrier_semaphore()

    for peer in peers:
        pl.semaphore_signal(barrier, inc=1, device_id={"batch": peer}, device_id_type=MESH)

    @pl.loop(1, feats)
    def _(k):
        pl.semaphore_signal(
            barrier, inc=1, device_id={"feat": (owner + k) % feats}, device_id_type=MESH
        )

    pl.semaphore_wait(barrier, len(peers) + feats - 1)

    lower, upper = pl.ds(0, half), pl.ds(half, half)
    moves = {}

    def own(v, link, part_of):
        index = link * 2 + part_of
        span = (lower, upper)[part_of]
        moves[v, link, part_of] = send(
            views[v].at[span], raw.at[v, link, span],
            g_send.at[v, index], g_recv.at[v, index], {"batch": peers[link]},
        )

    def forward(v):
        for link, part_of in ((0, 0), (1, 1)):
            moves[v, link, part_of].wait_recv()
            span = (lower, upper)[part_of]
            moves[v, 2, part_of] = send(
                raw.at[v, link, span], raw.at[v, 2, span],
                g_send.at[v, 4 + part_of], g_recv.at[v, 4 + part_of],
                {"batch": peers[1 - link]},
            )

    loads[0].wait()
    own(0, 0, 0)
    own(0, 1, 1)
    loads[1].wait()

    means = column_sums(
        rows, cols, 2,
        lambda r: tuple(x[r].astype(jnp.float32) for x in views),
    )
    means = tuple(m / rows for m in means)

    def squares(r):
        shifted = tuple(x[r].astype(jnp.float32) - m for x, m in zip(views, means))
        return tuple(s * s for s in shifted)

    spreads = column_sums(rows, cols, 2, squares)
    stats[0, 0:1] = means[0]
    stats[0, 1:2] = means[1]
    stats[0, 2:3] = spreads[0]
    stats[0, 3:4] = spreads[1]
    stat_moves = [
        send(stats.at[0], stats.at[k + 1], s_send.at[k], s_recv.at[k], {"batch": peers[k]})
        for k in range(3)
    ]
    own(0, 0, 1)
    own(0, 1, 0)
    for move in stat_moves:
        move.wait_recv()

    def merged(row):
        first = [stats[k, row : row + 1] for k in range(4)]
        return first, (first[0] + first[1]) + (first[2] + first[3])

    centers, factors = [], []
    for v in range(2):
        each, total = merged(v)
        center = total / groups
        gaps = [(e - center) * (e - center) for e in each]
        gap = (gaps[0] + gaps[1]) + (gaps[2] + gaps[3])
        variance = (merged(2 + v)[1] + rows * gap) / samples
        centers.append(center)
        factors.append(lax.rsqrt(variance + variance_floor))

    def normalize(v, slot, part_of=None):
        source = views[v] if slot == 0 else raw.at[v, slot - 1]
        count, base = (rows, 0) if part_of is None else (half, part_of * half)

        @pl.loop(0, count // 16, unroll=4)
        def _(i):
            r = pl.ds(pl.multiple_of(base + i * 16, 16), 16)
            values = source[r].astype(jnp.float32)
            low[v, slot, r] = ((values - centers[v]) * factors[v]).astype(jnp.bfloat16)

    ring = {}

    def buffers(v, slot):
        p = v * 4 + slot
        if slot == 0:
            return p, sum0.at[v], in0.at[v], gram0.at[v]
        return p, sum1.at[v, slot - 1], in1.at[v, slot - 1], gram.at[v, slot]

    def product(v, slot):
        p = v * 4 + slot
        part[p] = lax.dot_general(
            low[v, 0], low[v, slot], ROWS_T, preferred_element_type=jnp.float32
        )
        ring["pair", p] = send(
            part.at[p, theirs], pair_in.at[p], p_send.at[p], p_recv.at[p], {"feat": partner}
        )

    def scatter(v, slot):
        p, total, arrivals, _ = buffers(v, slot)
        ring["pair", p].wait_recv()
        total[...] = (part[p, mine] + pair_in[p]).astype(total.dtype)
        for k in range(1, depth):
            target = (z + k) % depth
            ring["sum", p, k] = send(
                total.at[pl.ds(pl.multiple_of(target * share, share), share)],
                arrivals.at[k - 1], z_send.at[p, k - 1], z_recv.at[p, k - 1],
                {"feat": target * 2 + core},
            )

    def collect(v, slot):
        p, total, arrivals, result = buffers(v, slot)
        value = total[pl.ds(pl.multiple_of(z * share, share), share)].astype(jnp.float32)
        for k in range(1, depth):
            ring["sum", p, k].wait_recv()
            value = value + arrivals[k - 1].astype(jnp.float32)
        span = pl.ds(pl.multiple_of(core * half + z * share, share), share)
        result[span] = value.astype(result.dtype)
        for k in range(1, depth):
            ring["all", p, k] = send(
                result.at[span], result.at[span], w_send.at[p, k - 1], w_recv.at[p, k - 1],
                {"feat": (z + k) % depth * 2 + core},
            )

    def swap(v, slot):
        p, _, _, result = buffers(v, slot)
        for k in range(1, depth):
            ring["all", p, k].wait_recv()
        ring["swap", p] = send(
            result.at[mine], result.at[mine], q_send.at[p], q_recv.at[p], {"feat": partner}
        )

    def finish(v, slot):
        ring["swap", v * 4 + slot].wait_recv()
        if slot == 0:
            high = gram0[v].astype(jnp.bfloat16)
            gram[v, 0] = high
            rest0[v] = (gram0[v] - high.astype(jnp.float32)).astype(jnp.bfloat16)

    def term(slot):
        return lambda r: (
            low[0, slot, r].astype(jnp.float32) * low[1, slot, r].astype(jnp.float32),
        )

    def diagonal_sum(slot):
        return column_sums(rows, cols, 1, term(slot))[0]

    width = min(256, cols)

    def spread(v, slots, add):
        other = 1 - v

        @pl.loop(0, cols // width)
        def _(i):
            c = pl.ds(pl.multiple_of(i * width, width), width)
            if add:
                total = grads[other][:, c]
            else:
                total = jnp.dot(rest0[v], low[other, 0, :, c], preferred_element_type=jnp.float32)
            for slot in slots:
                total = total + jnp.dot(
                    gram[v, slot], low[other, slot, :, c], preferred_element_type=jnp.float32
                )
            grads[other][:, c] = total

    def gram_product(slot):
        def body(r):
            if slot == 0:
                return (gram0[0, r] * gram0[1, r],)
            return (gram[0, slot, r].astype(jnp.float32) * gram[1, slot, r].astype(jnp.float32),)

        return column_sums(rows, rows, 1, body)[0]

    forward(0)
    for link, part_of in ((0, 0), (1, 1), (0, 1), (1, 0)):
        own(1, link, part_of)
    normalize(0, 0)
    product(0, 0)
    normalize(1, 0)
    product(1, 0)
    normalize(0, 1, 0)
    normalize(0, 2, 1)
    scatter(0, 0)
    scatter(1, 0)
    moves[0, 0, 1].wait_recv()
    normalize(0, 1, 1)
    product(0, 1)
    moves[0, 1, 0].wait_recv()
    normalize(0, 2, 0)
    product(0, 2)
    collect(0, 0)
    collect(1, 0)
    scatter(0, 1)
    scatter(0, 2)
    moves[0, 2, 0].wait_recv()
    moves[0, 2, 1].wait_recv()
    normalize(0, 3)
    product(0, 3)
    swap(0, 0)
    swap(1, 0)
    collect(0, 1)
    collect(0, 2)
    scatter(0, 3)
    finish(0, 0)
    finish(1, 0)
    forward(1)
    normalize(1, 1, 0)
    normalize(1, 2, 1)
    swap(0, 1)
    swap(0, 2)
    collect(0, 3)
    diagonal = diagonal_sum(0)
    square = gram_product(0)
    finish(0, 1)
    finish(0, 2)
    moves[1, 0, 1].wait_recv()
    normalize(1, 1, 1)
    product(1, 1)
    moves[1, 1, 0].wait_recv()
    normalize(1, 2, 0)
    product(1, 2)
    swap(0, 3)
    scatter(1, 1)
    scatter(1, 2)
    diagonal = diagonal + diagonal_sum(1) + diagonal_sum(2)
    finish(0, 3)
    spread(0, range(3), False)
    moves[1, 2, 0].wait_recv()
    moves[1, 2, 1].wait_recv()
    normalize(1, 3)
    product(1, 3)
    collect(1, 1)
    collect(1, 2)
    diagonal = (diagonal + diagonal_sum(3)) / samples
    missing = 1.0 - diagonal
    on_diagonal = jnp.sum(missing * missing - redundancy * diagonal * diagonal)
    scatter(1, 3)
    losses[owner] = jnp.full((8, 128), on_diagonal, jnp.float32)

    @pl.loop(1, feats)
    def _(k):
        pltpu.make_async_remote_copy(
            src_ref=losses.at[owner], dst_ref=losses.at[owner],
            send_sem=l_send, recv_sem=l_recv,
            device_id={"feat": (owner + k) % feats}, device_id_type=MESH,
        ).start()

    ddiag = (2.0 * (diagonal - 1.0)).astype(jnp.bfloat16).astype(jnp.float32)
    rest = ddiag - 2.0 * redundancy * diagonal
    scale = 2.0 * redundancy / samples
    final_moves = {}

    def reduce_final(v):
        def body(r):
            dnorm = scale * grads[v][r] + low[1 - v, 0, r].astype(jnp.float32) * rest
            normed = (views[v][r].astype(jnp.float32) - centers[v]) * factors[v]
            grads[v][r] = dnorm
            return dnorm, dnorm * normed

        first, second = column_sums(rows, cols, 2, body)
        finals[v, 0, 0:1] = first
        finals[v, 0, 1:2] = second

    def exchange_final(v):
        for k in range(3):
            final_moves[v, k] = send(
                finals.at[v, 0], finals.at[v, k + 1], f_send.at[v, k], f_recv.at[v, k],
                {"batch": peers[k]},
            )

    def merge_final(v, count):
        for k in range(3):
            final_moves[v, k].wait_recv()
        return tuple(
            (finals[v, 0, i : i + 1] + finals[v, 1, i : i + 1])
            + (finals[v, 2, i : i + 1] + finals[v, 3, i : i + 1])
            for i in range(count)
        )

    spread(0, (3,), True)
    collect(1, 3)
    swap(1, 1)
    swap(1, 2)
    reduce_final(1)
    exchange_final(1)
    finish(1, 1)
    finish(1, 2)
    spread(1, range(3), False)
    swap(1, 3)
    square = square + gram_product(1) + gram_product(2)
    rest_of = losses.at[pl.ds(0, feats - 1)]
    pltpu.make_async_copy(rest_of, rest_of, l_recv).wait()
    on_diagonal_all = jnp.sum(losses[...], axis=0)[0:1, 0:1]
    finish(1, 3)
    spread(1, (3,), True)
    reduce_final(0)
    square = square + gram_product(3)
    loss_part = redundancy * jnp.sum(square) / (samples * samples) + on_diagonal_all / groups
    finals[0, 0, 2:3] = jnp.broadcast_to(loss_part, (1, cols))
    exchange_final(0)
    for v in (1, 0):
        table[4 * v : 4 * v + 1] = centers[v]
        table[4 * v + 1 : 4 * v + 2] = factors[v]
    pltpu.make_async_copy(rest_of, rest_of, l_send).wait()
    for v in (1, 0):
        sums = merge_final(v, 3 - v)
        table[4 * v + 2 : 4 * v + 3] = sums[0] / samples
        table[4 * v + 3 : 4 * v + 4] = sums[1] / samples
        if v == 0:
            table[8:9] = sums[2] / features
    for copy in sent:
        copy.wait_send()


def last_step(table, dnorm_a, dnorm_b, view_a, view_b, loss, grad_a, grad_b):
    rows = view_a.shape[0]
    for v, (dnorm, view, grad) in enumerate(((dnorm_a, view_a, grad_a), (dnorm_b, view_b, grad_b))):
        center, factor, first, second = (table[4 * v + i : 4 * v + i + 1] for i in range(4))

        @pl.loop(0, rows // 16, unroll=4)
        def _(i):
            r = pl.ds(pl.multiple_of(i * 16, 16), 16)
            normed = (view[r].astype(jnp.float32) - center) * factor
            grad[r] = (dnorm[r] - first - normed * second) * factor

    loss[...] = table[8:9, 0:1]


def local(feats, view_a, view_b):
    rows, cols = view_a.shape
    half, depth = rows // 2, feats // 2
    share = half // depth
    f32, bf16 = jnp.float32, jnp.bfloat16
    dma = pltpu.SemaphoreType.DMA
    vmem = pl.BlockSpec(memory_space=pltpu.VMEM)
    table, dnorm_a, dnorm_b = pl.pallas_call(
        functools.partial(kernel, feats),
        out_shape=(
            jax.ShapeDtypeStruct((16, cols), f32),
            jax.ShapeDtypeStruct((rows, cols), f32),
            jax.ShapeDtypeStruct((rows, cols), f32),
        ),
        in_specs=[pl.BlockSpec(memory_space=pltpu.HBM)] * 2,
        out_specs=(vmem, vmem, vmem),
        scratch_shapes=[
            pltpu.VMEM((rows, cols), bf16),
            pltpu.VMEM((rows, cols), bf16),
            dma((2,)),
            pltpu.VMEM((2, 3, rows, cols), bf16),
            pltpu.VMEM((2, 4, rows, cols), bf16),
            pltpu.VMEM((8, rows, rows), f32),
            pltpu.VMEM((8, half, rows), f32),
            pltpu.VMEM((2, half, rows), f32),
            pltpu.VMEM((2, depth - 1, share, rows), f32),
            pltpu.VMEM((2, 3, half, rows), bf16),
            pltpu.VMEM((2, 3, depth - 1, share, rows), bf16),
            pltpu.VMEM((2, rows, rows), f32),
            pltpu.VMEM((2, 4, rows, rows), bf16),
            pltpu.VMEM((2, rows, rows), bf16),
            pltpu.VMEM((4, 4, cols), f32),
            pltpu.VMEM((2, 4, 4, cols), f32),
            pltpu.VMEM((feats, 8, 128), f32),
            dma((2, 6)), dma((2, 6)), dma((3,)), dma((3,)),
            dma((8,)), dma((8,)), dma((8, depth - 1)), dma((8, depth - 1)),
            dma((8, depth - 1)), dma((8, depth - 1)), dma((8,)), dma((8,)),
            dma((2, 3)), dma((2, 3)), dma, dma,
        ],
        compiler_params=pltpu.CompilerParams(
            collective_id=0, has_side_effects=True, vmem_limit_bytes=20 * 1024 * 1024
        ),
        name="twins",
    )(view_a, view_b)

    loss, grad_a, grad_b = pl.pallas_call(
        last_step,
        out_shape=(
            jax.ShapeDtypeStruct((1, 1), f32),
            jax.ShapeDtypeStruct((rows, cols), f32),
            jax.ShapeDtypeStruct((rows, cols), f32),
        ),
        in_specs=[vmem] * 5,
        out_specs=(vmem, vmem, vmem),
        compiler_params=pltpu.CompilerParams(vmem_limit_bytes=16 * 1024 * 1024),
        name="last_step",
    )(table, dnorm_a, dnorm_b, view_a, view_b)
    return loss[0, 0], grad_a, grad_b


def solution(mesh):
    feats = mesh.shape["feat"]
    body = functools.partial(local, feats) if mesh.shape["batch"] == 4 else plain
    return jax.shard_map(
        body,
        mesh=mesh,
        in_specs=(P("batch", "feat"), P("batch", "feat")),
        out_specs=(P(), P("batch", "feat"), P("batch", "feat")),
        check_vma=False,
    )
```
